128 devices in a mesh: section: 8 (over x, core), expert: 4 (over y), dp: 4 (over z).
Axes of the slice: x: 4, y: 4, z: 4, core: 2. Of those that a mesh axis runs over, the one named last changes fastest.
Arguments:
- x_in: bfloat16 [8, 256, 2048], P(None, ('expert', 'dp'), 'section'), may hold values from -6 to 6
- cotangent: bfloat16 [8, 256, 2048], P(None, ('expert', 'dp'), 'section'), may hold values from -6 to 6
- route_ids: int32 [8, 8, 256, 2], P('section', None, ('expert', 'dp')), may hold values from 0 to 15, all different within a row; in each aligned block of 16 rows (0 to 15, 16 to 31, ..., all dimensions but the last counted through in order) at most 2 rows name the same one
- norm_gain: float32 [8, 2048], P('section'), may hold values from 0.5 to 1.5
- router: bfloat16 [8, 2048, 16], P('section'), may hold values from -0.125 to 0.125
- w_gate_up: bfloat16 [8, 16, 2048, 1024], P('section', ('expert', 'dp')), may hold values from -0.125 to 0.125
- w_down: bfloat16 [8, 16, 512, 2048], P('section', ('expert', 'dp')), may hold values from -0.25 to 0.25
Outputs:
- grad_in: bfloat16 [8, 256, 2048], P(None, ('expert', 'dp'), 'section')
- grad_gate_up: float32 [8, 16, 2048, 1024], P('section', ('expert', 'dp'))
- grad_down: float32 [8, 16, 512, 2048], P('section', ('expert', 'dp'))
- grad_router: float32 [8, 2048, 16], P('section')
- grad_gain: float32 [8, 2048], P('section')
The draws below stay inside these ranges and needn't reach their ends.
Inputs may be any that keep to these rules, and one draw needn't show every extreme that they name: `route_ids`: each row names two different experts; the 16 rows of one device in one layer and micro-batch name any expert at most 2 times, a bound that some block reaches in some of them.
All inputs are finite; a program needn't handle non-finite values.
Results may differ from the reference program's by a relative error of at most 0.035.
Values may be sent and summed in bfloat16 or wider, within the bound.
No kernel may reach another device: no remote copies, remote signals or barrier semaphores. Data moves between devices by JAX's collectives and lax.ppermute only.
A program may use at most 64 MiB of HBM per device.

```python
import math
import jax
import jax.numpy as jnp
import numpy as np
from jax import lax

D = 2048
FFW = 512
TOP = 2
MICRO = 8
TOK_DEV = 16
EXPERTS = 16
CAP = 2
ROWS = 256
SECTIONS = 8


def shard_levels(own_key, shape, pieces, low, high):
    def one(axis_at, blocks):
        heights = jax.random.uniform(jax.random.fold_in(jax.random.fold_in(own_key, 6), axis_at), (blocks,), jnp.float32, low / len(pieces), high / len(pieces))
        return jnp.repeat(jnp.exp(heights), shape[axis_at] // blocks).reshape((-1,) + (1,) * (len(shape) - axis_at - 1))

    level = one(*pieces[0])
    for cut in pieces[1:]:
        level = level * one(*cut)
    return level


def routed_block(key, own, number, rows, count, top, reach, lean):
    sequence = jax.random.permutation(key, count)
    packed, ordinary = shares(count, rows * top, reach, lean, True), shares(count, rows * top, reach, lean, False)
    places = jnp.arange(count)

    def named(lengths, turn):
        used = int((lengths > 0).sum())
        fixed = max(1, used // 4)
        moved = fixed + (places - fixed + turn * (used - fixed)) % max(1, count - fixed)
        return jnp.zeros((count,), jnp.int32).at[sequence[jnp.where(places < fixed, places, moved)]].set(jnp.asarray(lengths, jnp.int32))

    lengths = jnp.where(number % 4 == 0, named(packed, number // 4), named(ordinary, number - number // 4 - 1))
    mixed = jax.random.permutation(jax.random.fold_in(own, 3), count)
    donor, taker = mixed[0:count // 2 * 2:2], mixed[1:count // 2 * 2:2]
    slack = jnp.minimum(lengths[donor] - 1, reach - lengths[taker]) // 2
    slack = jnp.where((donor == sequence[0]) | (taker == sequence[0]) | (lengths[taker] == 0), 0, jnp.maximum(slack, 0))
    moved = jax.random.randint(jax.random.fold_in(own, 4), (count // 2,), 0, 1 << 20) % (slack + 1)
    lengths = lengths.at[donor].add(-moved).at[taker].add(moved)
    items = jnp.searchsorted(jnp.cumsum(lengths), jnp.arange(rows * top), side="right").astype(jnp.int32)
    listing = items.reshape(top, rows).T
    listing = listing[jax.random.permutation(jax.random.fold_in(own, 1), rows)]
    turn = jax.random.randint(jax.random.fold_in(own, 2), (rows, 1), 0, top)
    return jnp.take_along_axis(listing, (jnp.arange(top)[None, :] + turn) % top, axis=1)


def shares(count, total, bound, slope, full):
    portions = [(1 << 20) // math.isqrt(rank ** slope) + 1 for rank in range(1, count + 1)]
    largest = bound if full else min(bound, max(-(-total // count), total * portions[0] // sum(portions)))
    least = 1 if total - largest >= count - 1 else 0
    holding, rest = [largest] + [least] * (count - 1), total - largest - least * (count - 1)
    while rest > 0:
        candidates = [i for i in range(1, count) if holding[i] < largest] or [i for i in range(1, count) if holding[i] < bound]
        mass, budget = sum([portions[i] for i in candidates]), rest
        for i in candidates:
            addition = min(bound - holding[i], max(1, budget * portions[i] // mass), rest)
            holding[i] = holding[i] + addition
            rest = rest - addition
    return np.array(holding)


def gaussian(stream_key, dims, width, limit, shards=(), kind=jnp.bfloat16):
    array = jax.random.normal(stream_key, dims, jnp.float32) * width
    if len(shards) > 0:
        array = shard_levels(stream_key, dims, shards, -0.22, 0.18) * array
    return jnp.clip(array, min=-limit, max=limit).astype(kind)


def setup_inputs(seed: int = 0) -> dict:
    arg_keys = jax.random.split(jax.random.key(seed), 8)
    x_in = gaussian(arg_keys[0], (MICRO, ROWS, D), 1.0, 6.0, ((1, 16), (2, 8)))
    cotangent = gaussian(arg_keys[1], (MICRO, ROWS, D), 1.0, 6.0, ((1, 16), (2, 8)))
    route_ids_keys = jax.random.split(jax.random.fold_in(arg_keys[2], 1), SECTIONS * MICRO * ROWS // TOK_DEV)
    route_ids_turns = jax.random.permutation(jax.random.fold_in(arg_keys[2], 3), SECTIONS * MICRO * ROWS // TOK_DEV)
    route_ids = jax.vmap(lambda own, number: routed_block(jax.random.fold_in(arg_keys[2], 2), own, number, TOK_DEV, EXPERTS, TOP, CAP, 2))(route_ids_keys, route_ids_turns).reshape((SECTIONS, MICRO, ROWS, TOP))
    norm_gain = jnp.clip(1.0 + 0.1 * jax.random.normal(arg_keys[3], (SECTIONS, D), jnp.float32), 0.5, 1.5)
    router = gaussian(arg_keys[4], (SECTIONS, D, EXPERTS), D ** -0.5, 0.125, ((0, 8),))
    w_gate_up = gaussian(arg_keys[5], (SECTIONS, EXPERTS, D, 2 * FFW), D ** -0.5, 0.125, ((0, 8), (1, 16)))
    w_down = gaussian(arg_keys[6], (SECTIONS, EXPERTS, FFW, D), FFW ** -0.5, 0.25, ((0, 8), (1, 16)))
    return dict(x_in=x_in, cotangent=cotangent, route_ids=route_ids, norm_gain=norm_gain, router=router, w_gate_up=w_gate_up, w_down=w_down)


EPS = 1e-05

def rounded(value):
    return lax.optimization_barrier(value.astype(jnp.bfloat16))

def slot_tables(route_rows):
    experts = jnp.arange(EXPERTS, dtype=jnp.int32)
    expert_hits = (route_rows[..., None] == experts).astype(jnp.int32)
    per_expert = lax.optimization_barrier(jnp.sum(expert_hits, axis=-2))
    before = jnp.cumsum(per_expert, axis=-2) - per_expert
    slot_ids = lax.optimization_barrier(jnp.sum(expert_hits * before[..., None, :], axis=-1))
    dest_cell = route_rows * CAP + slot_ids
    cell_ids = jnp.arange(EXPERTS * CAP, dtype=jnp.int32)
    slot_place = (dest_cell[..., None] == cell_ids).astype(jnp.float32)
    return (expert_hits.astype(jnp.float32), slot_place)

def layer_state(layer_in, route_rows, gain_vec, router_mat, w_gu):
    blocks = ROWS // TOK_DEV
    h_wide = layer_in.reshape(MICRO, blocks, TOK_DEV, D).astype(jnp.float32)
    inv_rms = lax.rsqrt(lax.optimization_barrier(jnp.mean(h_wide * h_wide, axis=-1, keepdims=True)) + EPS)
    normed = rounded(h_wide * inv_rms * gain_vec).astype(jnp.float32)
    expert_hits, slot_place = slot_tables(route_rows.reshape(MICRO, blocks, TOK_DEV, TOP))
    logits = jnp.einsum('mbtd,de->mbte', normed, router_mat.astype(jnp.float32), precision=lax.Precision.HIGHEST)
    chosen = lax.optimization_barrier(jnp.sum(expert_hits * logits[..., None, :], axis=-1))
    first_gate = jax.nn.sigmoid(chosen[..., 0] - chosen[..., 1])
    second_gate = jax.nn.sigmoid(chosen[..., 1] - chosen[..., 0])
    exp_rows = rounded(jnp.einsum('mbtkc,mbtd->mbcd', slot_place, normed, precision=lax.Precision.HIGHEST))
    exp_rows = exp_rows.astype(jnp.float32).reshape(MICRO, blocks, EXPERTS, CAP, D)
    gate_up = jnp.einsum('mbecd,edf->mbecf', exp_rows, w_gu.astype(jnp.float32), precision=lax.Precision.HIGHEST)
    gate_part = gate_up[..., :FFW]
    up_part = gate_up[..., FFW:]
    sigmoid_gate = jax.nn.sigmoid(gate_part)
    hidden = rounded(gate_part * sigmoid_gate * up_part).astype(jnp.float32)
    return (h_wide, inv_rms, normed, expert_hits, slot_place, first_gate, second_gate, exp_rows, gate_part, up_part, sigmoid_gate, hidden)

def expert_out(hidden, w_dn):
    blocks = ROWS // TOK_DEV
    out_rows = rounded(jnp.einsum('mbecf,efd->mbecd', hidden, w_dn.astype(jnp.float32), precision=lax.Precision.HIGHEST))
    return out_rows.astype(jnp.float32).reshape(MICRO, blocks, EXPERTS * CAP, D)

def forward_layer(layer_in, route_rows, gain_vec, router_mat, w_gu, w_dn):
    state = layer_state(layer_in, route_rows, gain_vec, router_mat, w_gu)
    h_wide, slot_place, first_gate, second_gate, hidden = (state[0], state[4], state[5], state[6], state[11])
    picked = jnp.einsum('mbtkc,mbcd->mbtkd', slot_place, expert_out(hidden, w_dn), precision=lax.Precision.HIGHEST)
    layer_out = h_wide + first_gate[..., None] * picked[..., 0, :] + second_gate[..., None] * picked[..., 1, :]
    return layer_out.astype(jnp.bfloat16).reshape(MICRO, ROWS, D)

def backward_layer(layer_in, grad_top, route_rows, gain_vec, router_mat, w_gu, w_dn):
    blocks = ROWS // TOK_DEV
    h_wide, inv_rms, normed, expert_hits, slot_place, first_gate, second_gate, exp_rows, gate_part, up_part, sigmoid_gate, hidden = layer_state(layer_in, route_rows, gain_vec, router_mat, w_gu)
    grad_wide = grad_top.reshape(MICRO, blocks, TOK_DEV, D).astype(jnp.float32)
    gates = jnp.stack([first_gate, second_gate], axis=-1)
    scaled = rounded(gates[..., None] * grad_wide[..., None, :]).astype(jnp.float32)
    dy_rows = rounded(jnp.einsum('mbtkc,mbtkd->mbcd', slot_place, scaled, precision=lax.Precision.HIGHEST))
    dy_rows = dy_rows.astype(jnp.float32).reshape(MICRO, blocks, EXPERTS, CAP, D)
    d_hidden = jnp.einsum('mbecd,efd->mbecf', dy_rows, w_dn.astype(jnp.float32), precision=lax.Precision.HIGHEST)
    silu_gate = gate_part * sigmoid_gate
    silu_slope = sigmoid_gate * (1.0 + gate_part * (1.0 - sigmoid_gate))
    gate_up_grad = rounded(jnp.concatenate([d_hidden * up_part * silu_slope, d_hidden * silu_gate], axis=-1))
    gate_up_grad = gate_up_grad.astype(jnp.float32)
    rows_grad = rounded(jnp.einsum('mbecf,edf->mbecd', gate_up_grad, w_gu.astype(jnp.float32), precision=lax.Precision.HIGHEST))
    rows_grad = rows_grad.astype(jnp.float32).reshape(MICRO, blocks, EXPERTS * CAP, D)
    grad_gu = jnp.einsum('mbecd,mbecf->edf', exp_rows, gate_up_grad, precision=lax.Precision.HIGHEST)
    grad_dn = jnp.einsum('mbecf,mbecd->efd', hidden, dy_rows, precision=lax.Precision.HIGHEST)
    normed_grad = jnp.einsum('mbtkc,mbcd->mbtd', slot_place, rows_grad, precision=lax.Precision.HIGHEST)
    picked = jnp.einsum('mbtkc,mbcd->mbtkd', slot_place, expert_out(hidden, w_dn), precision=lax.Precision.HIGHEST)
    gate_grad = lax.optimization_barrier(jnp.sum(grad_wide[..., None, :] * picked, axis=-1))
    logit_grad = first_gate * second_gate * (gate_grad[..., 0] - gate_grad[..., 1])
    logit_cols = logit_grad[..., None] * (expert_hits[..., 0, :] - expert_hits[..., 1, :])
    normed_grad = normed_grad + jnp.einsum('mbte,de->mbtd', logit_cols, router_mat.astype(jnp.float32), precision=lax.Precision.HIGHEST)
    grad_rt = jnp.einsum('mbtd,mbte->de', normed, logit_cols, precision=lax.Precision.HIGHEST)
    grad_gn = lax.optimization_barrier(jnp.sum(normed_grad * h_wide * inv_rms, axis=(0, 1, 2)))
    scaled_grad = normed_grad * gain_vec
    projection = lax.optimization_barrier(jnp.mean(scaled_grad * h_wide, axis=-1, keepdims=True))
    input_grad = grad_wide + inv_rms * scaled_grad - h_wide * inv_rms * inv_rms * inv_rms * projection
    return (input_grad.astype(jnp.bfloat16).reshape(MICRO, ROWS, D), (grad_gu, grad_dn, grad_rt, grad_gn))

def reference(x_in, cotangent, route_ids, norm_gain, router, w_gate_up, w_down):

    def forward_step(layer_in, params):
        route_rows, gain_vec, router_mat, w_gu, w_dn = params
        return (forward_layer(layer_in, route_rows, gain_vec, router_mat, w_gu, w_dn), layer_in)
    _, inputs = lax.scan(forward_step, x_in, (route_ids, norm_gain, router, w_gate_up, w_down))

    def backward_step(grad_top, params):
        route_rows, gain_vec, router_mat, w_gu, w_dn, layer_in = params
        return backward_layer(layer_in, grad_top, route_rows, gain_vec, router_mat, w_gu, w_dn)
    grad_in, grad_list = lax.scan(backward_step, cotangent, (route_ids, norm_gain, router, w_gate_up, w_down, inputs), reverse=True)
    return (grad_in, grad_list[0], grad_list[1], grad_list[2], grad_list[3])
```

```python
import jax
import jax.numpy as jnp
from jax import lax
from jax.sharding import PartitionSpec as P

EPS = 1e-05
ED = ("expert", "dp")


def swapped(value):
    count = lax.axis_size("section")
    return lax.ppermute(value, "section", [(s, s ^ 1) for s in range(count)])


def rotated(value, steps):
    count = lax.axis_size("section")
    return lax.ppermute(value, "section", [(s, (s + steps) % count) for s in range(count)])


def exchanged(rows, axis):
    return lax.all_to_all(rows, axis, split_axis=0, concat_axis=0, tiled=True)


def chosen(first, mine, other):
    return (jnp.where(first, mine, other), jnp.where(first, other, mine))


def route_tables(route_rows, n_expert, capacity):
    micro_count, tok_rows, _ = route_rows.shape
    experts = jnp.arange(n_expert, dtype=jnp.int32)
    hits = (route_rows[..., None] == experts).astype(jnp.int32)
    per_expert = jnp.sum(hits, axis=2)
    before = jnp.cumsum(per_expert, axis=1) - per_expert
    slot_ids = jnp.sum(hits * before[:, :, None, :], axis=3)
    micro_ids = jnp.arange(micro_count, dtype=jnp.int32)[:, None, None]
    cell = (route_rows * micro_count + micro_ids) * capacity + slot_ids
    cell = jnp.transpose(cell, (2, 0, 1)).reshape(2 * micro_count * tok_rows)
    cell_ids = jnp.arange(n_expert * micro_count * capacity, dtype=jnp.int32)
    place = (cell[:, None] == cell_ids).astype(jnp.bfloat16)
    diff = (hits[:, :, 0, :] - hits[:, :, 1, :]).astype(jnp.float32)
    return place, diff.reshape(micro_count * tok_rows, n_expert)


def dot(a, b, dims):
    return lax.dot_general(a, b, (dims, ((), ())), preferred_element_type=jnp.float32)


def forward_layer(h, wt, n_rank):
    place, diff, gain, router, w_gu, w_dn = wt
    tokens, width = h.shape
    both = place[:tokens] + place[tokens:]
    h_wide = h.astype(jnp.float32)
    inv = lax.rsqrt(jnp.mean(h_wide * h_wide, axis=-1, keepdims=True) + EPS)
    u = (h_wide * inv * gain).astype(jnp.bfloat16)
    send = dot(both, u, ((0,), (0,))).astype(jnp.bfloat16)
    rows = exchanged(send.reshape(n_rank, -1, width), ED).reshape(-1, width)
    logits = dot(u, router, ((1,), (0,)))
    delta = jnp.sum(diff * logits, axis=1, keepdims=True)
    g1, g2 = jax.nn.sigmoid(delta), jax.nn.sigmoid(-delta)
    gate_up = dot(rows, w_gu, ((1,), (0,)))
    half = w_gu.shape[1] // 2
    a, b = gate_up[:, :half], gate_up[:, half:]
    sig = jax.nn.sigmoid(a)
    hidden = (a * sig * b).astype(jnp.bfloat16)
    out = dot(hidden, w_dn, ((1,), (0,))).astype(jnp.bfloat16)
    back = exchanged(out.reshape(n_rank, -1, width), ED).reshape(-1, width)
    y = dot(place, back, ((1,), (0,)))
    y1, y2 = y[:tokens], y[tokens:]
    h_next = (h_wide + g1 * y1 + g2 * y2).astype(jnp.bfloat16)
    saved = (h, inv, u, g1, g2, rows, gate_up, hidden, y.astype(jnp.bfloat16))
    return h_next, saved


def backward_layer(grad, wt, saved, n_rank):
    place, diff, gain, router, w_gu, w_dn = wt
    h, inv, u, g1, g2, rows, gate_up, hidden, y = saved
    tokens, width = h.shape
    both = place[:tokens] + place[tokens:]
    half = w_gu.shape[1] // 2
    h_wide = h.astype(jnp.float32)
    g_wide = grad.astype(jnp.float32)
    scaled = jnp.concatenate([(g1 * g_wide).astype(jnp.bfloat16), (g2 * g_wide).astype(jnp.bfloat16)], axis=0)
    dy_send = dot(place, scaled, ((0,), (0,))).astype(jnp.bfloat16)
    dy = exchanged(dy_send.reshape(n_rank, -1, width), ED).reshape(-1, width)
    c1 = jnp.sum(g_wide * y[:tokens].astype(jnp.float32), axis=-1, keepdims=True)
    c2 = jnp.sum(g_wide * y[tokens:].astype(jnp.float32), axis=-1, keepdims=True)
    logit_cols = g1 * g2 * (c1 - c2) * diff
    through_router = dot(logit_cols, router.astype(jnp.float32), ((1,), (1,)))
    router_part = dot(logit_cols, u.astype(jnp.float32), ((0,), (0,)))
    a, b = gate_up[:, :half], gate_up[:, half:]
    sig = jax.nn.sigmoid(a)
    d_hidden = dot(dy, w_dn, ((1,), (1,)))
    q = jnp.concatenate(
        [d_hidden * b * (sig * (1.0 + a * (1.0 - sig))), d_hidden * (a * sig)], axis=-1
    ).astype(jnp.bfloat16)
    du_rows = dot(q, w_gu, ((1,), (1,))).astype(jnp.bfloat16)
    back = exchanged(du_rows.reshape(n_rank, -1, width), ED).reshape(-1, width)
    du = dot(both, back, ((1,), (0,))) + through_router
    gain_part = jnp.sum(du * h_wide * inv, axis=0, keepdims=True)
    w = du * gain
    proj = jnp.mean(w * h_wide, axis=-1, keepdims=True)
    out = (g_wide + inv * w - h_wide * (inv * inv * inv) * proj).astype(jnp.bfloat16)
    return out, (dy, q, router_part, gain_part)


def local(x_in, cotangent, route_ids, norm_gain, router, w_gate_up, w_down):
    micro_count, tok_rows, cols = x_in.shape
    n_section = lax.axis_size("section")
    n_rank = lax.axis_size("expert") * lax.axis_size("dp")
    n_expert = router.shape[2]
    width = w_down.shape[3]
    half_micro = micro_count // 2
    stages = n_section // 2
    capacity = tok_rows * 2 // n_expert
    section = lax.axis_index("section")
    lane = section % 2
    stage = section // 2
    first = lane == 0

    x_lo, x_hi = x_in[:half_micro], x_in[half_micro:]
    c_lo, c_hi = cotangent[:half_micro], cotangent[half_micro:]
    sent = jnp.stack([x_lo, x_hi] * (n_section // 4) + [c_lo, c_hi] * (n_section // 4))
    landed = exchanged(sent, "section")
    seed = jnp.transpose(landed, (1, 2, 0, 3)).reshape(half_micro * tok_rows, width)

    own_gu, own_dn = w_gate_up[0, 0], w_down[0, 0]
    gu_a, gu_b = chosen(first, own_gu, swapped(own_gu))
    dn_a, dn_b = chosen(first, own_dn, swapped(own_dn))
    rt_a, rt_b = chosen(first, router[0], swapped(router[0]))
    gn_a, gn_b = chosen(first, norm_gain, swapped(norm_gain))
    id_a, id_b = chosen(first, route_ids[0], swapped(route_ids[0]))
    id_a, id_b = (lax.dynamic_slice_in_dim(r, lane * half_micro, half_micro, 0) for r in (id_a, id_b))
    wt_a = (*route_tables(id_a, n_expert, capacity), gn_a, rt_a, gu_a, dn_a)
    wt_b = (*route_tables(id_b, n_expert, capacity), gn_b, rt_b, gu_b, dn_b)

    h_in = seed
    for step in range(stages):
        h_mid, saved_a = forward_layer(h_in, wt_a, n_rank)
        if step + 1 < stages:
            h_out, saved_b = forward_layer(h_mid, wt_b, n_rank)
            h_in = jnp.where(stage == step + 1, rotated(h_out, 2), h_in)
        else:
            _, saved_b = forward_layer(h_mid, wt_b, n_rank)

    grad = seed
    for step in range(stages):
        mid, parts_b = backward_layer(grad, wt_b, saved_b, n_rank)
        low, parts_a = backward_layer(mid, wt_a, saved_a, n_rank)
        if step + 1 < stages:
            grad = jnp.where(stage == stages - 2 - step, rotated(low, -2), grad)

    pieces = jnp.transpose(low.reshape(half_micro, tok_rows, n_section, cols), (2, 0, 1, 3))
    landed = exchanged(pieces, "section")
    grad_in = jnp.concatenate([landed[0], landed[1]], axis=0)

    rows_mine, rows_other = chosen(first, saved_a[5], saved_b[5])
    hid_mine, hid_other = chosen(first, saved_a[7], saved_b[7])
    dy_mine, dy_other = chosen(first, parts_a[0], parts_b[0])
    q_mine, q_other = chosen(first, parts_a[1], parts_b[1])
    all_rows = jnp.concatenate([rows_mine, swapped(rows_other)], axis=0)
    all_hid = jnp.concatenate([hid_mine, swapped(hid_other)], axis=0)
    all_dy = jnp.concatenate([dy_mine, swapped(dy_other)], axis=0)
    all_q = jnp.concatenate([q_mine, swapped(q_other)], axis=0)
    grad_gu = dot(all_rows, all_q, ((0,), (0,)))
    grad_dn = dot(all_hid, all_dy, ((0,), (0,)))

    small_a = jnp.concatenate([parts_a[2], parts_a[3]], axis=0)
    small_b = jnp.concatenate([parts_b[2], parts_b[3]], axis=0)
    small_mine, small_other = chosen(first, small_a, small_b)
    small = (small_mine + swapped(small_other)).astype(jnp.bfloat16)
    copies = jnp.broadcast_to(small, (n_rank, *small.shape))
    total = jnp.sum(exchanged(copies, ED).astype(jnp.float32), axis=0)
    grad_router = jnp.transpose(total[:n_expert])
    grad_gain = total[n_expert]
    return (grad_in, grad_gu[None, None], grad_dn[None, None], grad_router[None], grad_gain[None])


def solution(mesh):
    in_specs = (
        P(None, ED, "section"),
        P(None, ED, "section"),
        P("section", None, ED, None),
        P("section", None),
        P("section", None, None),
        P("section", ED, None, None),
        P("section", ED, None, None),
    )
    out_specs = (
        P(None, ED, "section"),
        P("section", ED, None, None),
        P("section", ED, None, None),
        P("section", None, None),
        P("section", None),
    )
    return jax.shard_map(local, mesh=mesh, in_specs=in_specs, out_specs=out_specs, check_vma=False)
```
